32 devices in a mesh: shard: 8 (over z, y), model: 4 (over x, core).
Axes of the slice: x: 2, y: 2, z: 4, core: 2. Of those that a mesh axis runs over, the one named last changes fastest.
Arguments:
- gradients: float32 [32, 128, 4096], P(None, 'shard', 'model'), may hold values from -6 to 6
- momentum: float32 [32, 128, 4096], P(None, 'shard', 'model'), may hold values from -6 to 6
- weights: float32 [32, 128, 4096], P(None, 'shard', 'model'), may hold values from -0.1875 to 0.1875
Outputs:
- new_weights: float32 [32, 128, 4096], P(None, 'shard', 'model')
- new_momentum: float32 [32, 128, 4096], P(None, 'shard', 'model')
The draws below stay inside these ranges and needn't reach their ends.
All inputs are finite; a program needn't handle non-finite values.
Results may differ from the reference program's by a relative error of at most 0.00015.
Values sent between devices are 32-bit elements; how exact they have to be, the bound alone decides.
A program may use at most 128 MiB of HBM per device.

```python
import jax
import jax.numpy as jnp
from jax import lax

SIDE = 128
WIDE = 4096
MATS = 32
ITERS = 4


def level_of(stream_key, dims, cuts, low, top_value):
    def one(position, shards_of):
        steps = jax.random.uniform(jax.random.fold_in(jax.random.fold_in(stream_key, 6), position), (shards_of,), jnp.float32, low / len(cuts), top_value / len(cuts))
        return jnp.repeat(jnp.exp(steps), dims[position] // shards_of).reshape((-1,) + (1,) * (len(dims) - position - 1))

    level = one(*cuts[0])
    for cut in cuts[1:]:
        level = level * one(*cut)
    return level


def gaussian(rng, shape, width, reach, cuts=(), held_as=jnp.bfloat16):
    result = width * jax.random.normal(rng, shape, jnp.float32)
    if cuts:
        result = result * level_of(rng, shape, cuts, -0.22, 0.18)
    return jnp.clip(result, -reach, reach).astype(held_as)


def setup_inputs(seed: int = 0) -> dict:
    key_of = jax.random.split(jax.random.key(seed), 4)
    gradients = gaussian(key_of[0], (MATS, SIDE, WIDE), 1.0, 6.0, ((1, 8), (2, 4)), jnp.float32)
    momentum = gaussian(key_of[1], (MATS, SIDE, WIDE), 1.0, 6.0, ((1, 8), (2, 4)), jnp.float32)
    weights = gaussian(key_of[2], (MATS, SIDE, WIDE), 0.03, 0.1875, ((1, 8), (2, 4)), jnp.float32)
    return {"gradients": gradients, "momentum": momentum, "weights": weights}


hold_rate = 0.8
learn_rate = 1.0

def reference(gradients, momentum, weights):
    new_momentum = hold_rate * momentum + gradients

    def orthogonal_one(stack):
        iterate = stack[None]
        iterate = iterate * lax.rsqrt(lax.optimization_barrier(jnp.sum(iterate * iterate, axis=(1, 2), keepdims=True)) + 1e-06)
        for step in range(ITERS):
            gram = jnp.einsum('mik,mjk->mij', iterate, iterate, precision=lax.Precision.HIGHEST)
            mixed = -4.775 * gram + 2.0315 * jnp.einsum('mij,mjk->mik', gram, gram, precision=lax.Precision.HIGHEST)
            iterate = 3.4445 * iterate + jnp.einsum('mij,mjk->mik', mixed, iterate, precision=lax.Precision.HIGHEST)
        return iterate[0]
    iterate = lax.map(orthogonal_one, new_momentum)
    new_weights = weights - learn_rate * iterate
    return (new_weights, new_momentum)
```

```python
import functools

import jax
import jax.numpy as jnp
from jax import lax
from jax.experimental import pallas as pl
from jax.experimental.pallas import tpu as pltpu
from jax.sharding import PartitionSpec as P

ITERS = 4
MESH = pl.DeviceIdType.MESH
HIGHEST = lax.Precision.HIGHEST


hold_rate = 0.8
learn_rate = 1.0


def mm(a, b):
    return jnp.dot(a, b, precision=HIGHEST, preferred_element_type=jnp.float32)


def direction(gram):
    side = gram.shape[-1]
    row = lax.broadcasted_iota(jnp.int32, (side, side), 0)
    col = lax.broadcasted_iota(jnp.int32, (side, side), 1)
    diagonal = row == col
    squares = jnp.sum(jnp.where(diagonal, gram, 0.0), axis=(0, 1), keepdims=True)
    scale = lax.rsqrt(squares + 1e-06)
    a = gram * scale * scale
    q = jnp.where(diagonal, jnp.broadcast_to(scale, gram.shape), 0.0)
    for step in range(ITERS):
        mixed = -4.775 * a + 2.0315 * mm(a, a)
        if step == 0:
            q_next = 3.4445 * q + mixed * scale
        else:
            q_next = 3.4445 * q + mm(mixed, q)
        if step < ITERS - 1:
            half = 3.4445 * a + mm(mixed, a)
            a = 3.4445 * half + mm(mixed, half)
        q = q_next
    return q


def offsets(n):
    return sorted(range(1, n), key=lambda off: -min(off, n - off))


def exchange_kernel(n, k, x_ref, back_ref, held, result, grams,
                    f_send, f_recv, g_send, g_recv, b_send, b_recv, own_in, own_out):
    me = lax.axis_index("shard")
    col = lax.axis_index("model")
    local, _, rows, wide = held.shape
    side = n * rows

    def peer(off):
        return lax.rem(me + off, n)

    def forward(j, off):
        to = peer(off)
        return pltpu.make_async_remote_copy(
            src_ref=x_ref.at[to * local + j], dst_ref=held.at[j, me],
            send_sem=f_send.at[j, off], recv_sem=f_recv.at[j, off],
            device_id={"shard": to}, device_id_type=MESH)

    def share(j, off):
        return pltpu.make_async_remote_copy(
            src_ref=grams.at[j, col], dst_ref=grams.at[j, col],
            send_sem=g_send.at[j, off], recv_sem=g_recv.at[j, off],
            device_id={"model": lax.rem(col + off, k)}, device_id_type=MESH)

    def backward(j, off):
        to = peer(off)
        return pltpu.make_async_remote_copy(
            src_ref=result.at[j, to], dst_ref=back_ref.at[me * local + j],
            send_sem=b_send.at[j, off], recv_sem=b_recv.at[j, off],
            device_id={"shard": to}, device_id_type=MESH)

    def mine_in(j):
        return pltpu.make_async_copy(x_ref.at[me * local + j], held.at[j, me], own_in.at[j])

    def mine_out(j):
        return pltpu.make_async_copy(result.at[j, me], back_ref.at[me * local + j], own_out.at[j])

    barrier = pltpu.get_barrier_semaphore()
    for off in range(1, n):
        pl.semaphore_signal(barrier, inc=1, device_id={"shard": peer(off)}, device_id_type=MESH)
    for off in range(1, k):
        pl.semaphore_signal(barrier, inc=1, device_id={"model": lax.rem(col + off, k)}, device_id_type=MESH)
    pl.semaphore_wait(barrier, n + k - 2)

    @pl.loop(0, local)
    def _(j):
        for off in offsets(n):
            forward(j, off).start()
        mine_in(j).start()

    @pl.loop(0, local)
    def _(j):
        for off in offsets(n):
            forward(j, off).wait_recv()
        mine_in(j).wait()
        x = held[j].reshape(side, wide)
        grams[j, col] = lax.dot_general(
            x, x, (((1,), (1,)), ((), ())), precision=HIGHEST, preferred_element_type=jnp.float32)
        for off in range(1, k):
            share(j, off).start()
        for off in range(1, k):
            share(j, off).wait_recv()
        gram = grams[j, 0]
        for i in range(1, k):
            gram = gram + grams[j, i]
        result[j] = mm(direction(gram), x).reshape(n, rows, wide)
        for off in offsets(n):
            backward(j, off).start()
        mine_out(j).start()

    @pl.loop(0, local)
    def _(j):
        for off in range(1, n):
            forward(j, off).wait_send()
            backward(j, off).wait()
        for off in range(1, k):
            share(j, off).wait_send()
        mine_out(j).wait()


def by_kernel(n, k, x):
    mats, rows, wide = x.shape
    local = mats // n
    side = n * rows
    dma = pltpu.SemaphoreType.DMA
    return pl.pallas_call(
        functools.partial(exchange_kernel, n, k),
        out_shape=jax.ShapeDtypeStruct(x.shape, jnp.float32),
        in_specs=[pl.BlockSpec(memory_space=pl.ANY)],
        out_specs=pl.BlockSpec(memory_space=pl.ANY),
        scratch_shapes=[
            pltpu.VMEM((local, n, rows, wide), jnp.float32),
            pltpu.VMEM((local, n, rows, wide), jnp.float32),
            pltpu.VMEM((local, k, side, side), jnp.float32),
            dma((local, n)), dma((local, n)),
            dma((local, k)), dma((local, k)),
            dma((local, n)), dma((local, n)),
            dma((local,)), dma((local,)),
        ],
        compiler_params=pltpu.CompilerParams(
            collective_id=0, has_side_effects=True, vmem_limit_bytes=32 * 1024 * 1024),
    )(x)


def on_device(n, k, gradients, momentum, weights):
    new_momentum = hold_rate * momentum + gradients
    back = by_kernel(n, k, new_momentum)
    new_weights = weights - learn_rate * back
    return (new_weights, new_momentum)


def solution(mesh):
    placed = P(None, "shard", "model")
    return jax.shard_map(
        functools.partial(on_device, mesh.shape["shard"], mesh.shape["model"]),
        mesh=mesh,
        in_specs=(placed, placed, placed),
        out_specs=(placed, placed),
        check_vma=False,
    )
```

```python
import functools

import jax
import jax.numpy as jnp
from jax import lax
from jax.experimental import pallas as pl
from jax.experimental.pallas import tpu as pltpu
from jax.sharding import PartitionSpec as P

ITERS = 4
VMEM_LIMIT = 40 * 1024 * 1024
FINISH_LIMIT = 16 * 1024 * 1024
MESH = pl.DeviceIdType.MESH
HIGHEST = lax.Precision.HIGHEST


hold_rate = 0.8
learn_rate = 1.0


def mm(a, b):
    return jnp.dot(a, b, precision=HIGHEST, preferred_element_type=jnp.float32)


def direction(gram):
    side = gram.shape[-1]
    row = lax.broadcasted_iota(jnp.int32, (side, side), 0)
    col = lax.broadcasted_iota(jnp.int32, (side, side), 1)
    diagonal = row == col
    squares = jnp.sum(jnp.where(diagonal, gram, 0.0), axis=(0, 1), keepdims=True)
    scale = lax.rsqrt(squares + 1e-06)
    a = gram * scale * scale
    q = jnp.where(diagonal, jnp.broadcast_to(scale, gram.shape), 0.0)
    for step in range(ITERS):
        mixed = -4.775 * a + 2.0315 * mm(a, a)
        if step == 0:
            q_next = 3.4445 * q + mixed * scale
        else:
            q_next = 3.4445 * q + mm(mixed, q)
        if step < ITERS - 1:
            half = 3.4445 * a + mm(mixed, a)
            a = 3.4445 * half + mm(mixed, half)
        q = q_next
    return q


def partner(me, off, n):
    if n & (n - 1):
        return lax.rem(me + off, n)
    for bit in range(n.bit_length() - 1):
        if (off >> bit) & 1:
            me = me + (1 - 2 * ((me // (1 << bit)) % 2)) * (1 << bit)
    return me


def exchange_kernel(n, k, g_ref, m_ref, back_ref, new_ref, grad, moved, held, result, grams,
                    l_grad, l_moved, f_send, f_recv, g_send, g_recv, b_send, b_recv,
                    own_in, own_out, own_new):
    me = lax.axis_index("shard")
    col = lax.axis_index("model")
    local, _, rows, wide = held.shape
    side = n * rows

    def chunk(j):
        return pl.ds(j * n, n)

    def load_grad(j):
        return pltpu.make_async_copy(g_ref.at[chunk(j)], grad.at[j], l_grad.at[j])

    def load_moved(j):
        return pltpu.make_async_copy(m_ref.at[chunk(j)], moved.at[j], l_moved.at[j])

    def store_new(j):
        return pltpu.make_async_copy(moved.at[j], new_ref.at[chunk(j)], own_new.at[j])

    def forward(j, off):
        to = partner(me, off, n)
        return pltpu.make_async_remote_copy(
            src_ref=moved.at[j, to], dst_ref=held.at[j, me],
            send_sem=f_send.at[j, off], recv_sem=f_recv.at[j, off],
            device_id={"shard": to}, device_id_type=MESH)

    def share(j, off):
        return pltpu.make_async_remote_copy(
            src_ref=grams.at[j, col], dst_ref=grams.at[j, col],
            send_sem=g_send.at[j, off], recv_sem=g_recv.at[j, off],
            device_id={"model": partner(col, off, k)}, device_id_type=MESH)

    def backward(j, off):
        to = partner(me, off, n)
        return pltpu.make_async_remote_copy(
            src_ref=result.at[j, to], dst_ref=back_ref.at[j * n + me],
            send_sem=b_send.at[j, off], recv_sem=b_recv.at[j, off],
            device_id={"shard": to}, device_id_type=MESH)

    def mine_in(j):
        return pltpu.make_async_copy(moved.at[j, me], held.at[j, me], own_in.at[j])

    def mine_out(j):
        return pltpu.make_async_copy(result.at[j, me], back_ref.at[j * n + me], own_out.at[j])

    barrier = pltpu.get_barrier_semaphore()
    for off in range(n - 1, 0, -1):
        pl.semaphore_signal(barrier, inc=1, device_id={"shard": partner(me, off, n)}, device_id_type=MESH)
    for off in range(1, k):
        pl.semaphore_signal(barrier, inc=1, device_id={"model": partner(col, off, k)}, device_id_type=MESH)

    @pl.loop(0, local)
    def _(j):
        load_moved(j).start()
        load_grad(j).start()

    def step(j):
        load_moved(j).wait()
        load_grad(j).wait()
        moved[j] = hold_rate * moved[j] + grad[j]

    def send(j):
        for off in range(1, n):
            forward(j, off).start()
        mine_in(j).start()

    step(0)
    pl.semaphore_wait(barrier, n + k - 2)
    send(0)

    @pl.loop(1, local)
    def _(j):
        step(j)
        send(j)

    @pl.loop(0, local)
    def _(j):
        store_new(j).start()

    @pl.loop(0, local)
    def _(j):
        for off in range(1, n):
            forward(j, off).wait_recv()
        mine_in(j).wait()
        x = held[j].reshape(side, wide)
        grams[j, col] = lax.dot_general(
            x, x, (((1,), (1,)), ((), ())), precision=HIGHEST, preferred_element_type=jnp.float32)
        for off in range(1, k):
            share(j, off).start()
        for off in range(1, k):
            share(j, off).wait_recv()
        gram = grams[j, 0]
        for i in range(1, k):
            gram = gram + grams[j, i]
        result[j] = mm(direction(gram), x).reshape(n, rows, wide)
        for off in range(1, n):
            backward(j, off).start()
        mine_out(j).start()

    @pl.loop(0, local)
    def _(j):
        for off in range(1, n):
            forward(j, off).wait_send()
        for off in range(1, k):
            share(j, off).wait_send()
        store_new(j).wait()
        mine_out(j).wait()

    @pl.loop(0, local)
    def _(j):
        for off in range(1, n):
            backward(j, off).wait()


def by_kernel(n, k, gradients, momentum):
    mats, rows, wide = gradients.shape
    local = mats // n
    side = n * rows
    dma = pltpu.SemaphoreType.DMA
    whole = jax.ShapeDtypeStruct(gradients.shape, jnp.float32)
    return pl.pallas_call(
        functools.partial(exchange_kernel, n, k),
        out_shape=(whole, whole),
        in_specs=[pl.BlockSpec(memory_space=pltpu.HBM)] * 2,
        out_specs=[pl.BlockSpec(memory_space=pl.ANY)] * 2,
        scratch_shapes=[
            *[pltpu.VMEM((local, n, rows, wide), jnp.float32)] * 4,
            pltpu.VMEM((local, k, side, side), jnp.float32),
            dma((local,)), dma((local,)),
            dma((local, n)), dma((local, n)),
            dma((local, k)), dma((local, k)),
            dma((local, n)), dma((local, n)),
            dma((local,)), dma((local,)), dma((local,)),
        ],
        compiler_params=pltpu.CompilerParams(
            collective_id=0, has_side_effects=True, vmem_limit_bytes=VMEM_LIMIT),
    )(pltpu.with_memory_space_constraint(gradients, pltpu.HBM), pltpu.with_memory_space_constraint(momentum, pltpu.HBM))


def finish_kernel(pieces, back_ref, w_ref, new_ref, out_w, out_new, done, sem_w, sem_new):
    step = back_ref.shape[0] // pieces

    def part(i):
        return pl.ds(i * step, step)

    def put_new(i):
        return pltpu.make_async_copy(new_ref.at[part(i)], out_new.at[part(i)], sem_new.at[i])

    def put_w(i):
        return pltpu.make_async_copy(done.at[part(i)], out_w.at[part(i)], sem_w.at[i])

    for i in range(pieces):
        put_new(i).start()
    for i in range(pieces):
        done[part(i)] = w_ref[part(i)] - learn_rate * back_ref[part(i)]
        put_w(i).start()
    for i in range(pieces):
        put_new(i).wait()
        put_w(i).wait()


def finish(pieces, back, weights, new_momentum):
    whole = jax.ShapeDtypeStruct(back.shape, jnp.float32)
    hold = pl.BlockSpec(memory_space=pltpu.VMEM)
    leave = pl.BlockSpec(memory_space=pl.ANY)
    return pl.pallas_call(
        functools.partial(finish_kernel, pieces),
        out_shape=(whole, whole),
        in_specs=[hold, hold, leave],
        out_specs=[leave, leave],
        scratch_shapes=[
            pltpu.VMEM(back.shape, jnp.float32),
            pltpu.SemaphoreType.DMA((pieces,)), pltpu.SemaphoreType.DMA((pieces,)),
        ],
        compiler_params=pltpu.CompilerParams(vmem_limit_bytes=FINISH_LIMIT),
        cost_estimate=pl.CostEstimate(flops=2 * back.size, bytes_accessed=20 * back.size, transcendentals=0),
    )(back, weights, new_momentum)


def on_device(n, k, gradients, momentum, weights):
    back, new_momentum = by_kernel(n, k, gradients, momentum)
    return tuple(finish(n, back, weights, new_momentum))


def solution(mesh):
    placed = P(None, "shard", "model")
    return jax.shard_map(
        functools.partial(on_device, mesh.shape["shard"], mesh.shape["model"]),
        mesh=mesh,
        in_specs=(placed, placed, placed),
        out_specs=(placed, placed),
        check_vma=False,
    )
```
